256 devices in a mesh: energy: 64 (over y, x_lo, z), layer: 4 (over x_hi, core).
Axes of the slice: x: 4 (x_hi: 2, x_lo: 2; x = x_hi * 2 + x_lo), y: 4, z: 8, core: 2. Of those that a mesh axis runs over, the one named last changes fastest.
Arguments:
- layer_inverse: float32 [64, 32, 256, 256], P('energy', 'layer'), may hold values from -0.008125 to 1, as said below
- coupling: float32 [256, 256], replicated, may hold values from -0.5125 to 0.5125, as said below
- lead_left: float32 [64, 256, 256], P('energy'), may hold values from -0.0040625 to 0.5, as said below
- lead_right: float32 [64, 256, 256], P('energy'), may hold values from -0.0040625 to 0.5, as said below
- quad_weight: float32 [64], replicated, may hold values from 0.0015625 to 0.0625
- energy_slot: int32 [64], P('energy'), may hold values from 0 to 63, each once
- plane_of: int32 [32], replicated, may hold values from 0 to 1023
- doping: float32 [1024, 128, 128], P(('energy', 'layer')), may hold values from -6 to 6
- screening: float32 [1024, 128, 128], P(('energy', 'layer')), may hold values from 0.25 to 2
Outputs:
- layer_density: float32 [32, 256], P('layer')
- potential: float32 [1024, 128, 128], P(('energy', 'layer'))
- residual: float32 [1024, 128, 128], P(('energy', 'layer'))
The draws below stay inside these ranges and needn't reach their ends.
Inputs may be any that keep to these rules, and one draw needn't show every extreme that they name: `layer_inverse`: each block is symmetric; its diagonal entries lie between 0.3 and 1.0 and its other entries within 0.13 * 256 ** -0.5 of zero. `coupling`: entries are independent with mean zero. `lead_left`: each block is symmetric; its diagonal entries lie between 0.15 and 0.5 and its other entries within 0.065 * 256 ** -0.5 of zero. `lead_right`: each block is symmetric; its diagonal entries lie between 0.15 and 0.5 and its other entries within 0.065 * 256 ** -0.5 of zero. `energy_slot`: every quadrature index appears once. `plane_of`: several layers may share a plane.
All inputs are finite; a program needn't handle non-finite values.
Results may differ from the reference program's by a relative error of at most 0.00018.
Values sent between devices are 32-bit elements; how exact they have to be, the bound alone decides.
No kernel may reach another device: no remote copies, remote signals or barrier semaphores. Data moves between devices by JAX's collectives and lax.ppermute only.
A program may use at most 128 MiB of HBM per device.

```python
import math
from functools import partial
import jax
import jax.numpy as jnp
from jax import lax

M = 256
ORB_Y = 16
ORB_Z = 16
NY = 128
NZ = 128
LAYERS = 32
ENERGIES = 64
NX = 1024
CG_ITERS = 3


def symmetric_blocks(key, lead_shape, factor):
    key_diag, key_off = jax.random.split(key)
    orbitals = M
    diag_values = jnp.exp(jax.random.uniform(key_diag, lead_shape + (orbitals,), jnp.float32, math.log(0.3), 0.0))
    half_width = 0.13 * orbitals ** (-0.5)
    noise = jax.random.uniform(key_off, lead_shape + (orbitals, orbitals), jnp.float32, -half_width, half_width)
    noise = 0.5 * (noise + jnp.swapaxes(noise, -1, -2))
    identity_mat = jnp.eye(orbitals, dtype=jnp.float32)
    blocks = noise * (1.0 - identity_mat) + diag_values[..., None] * identity_mat
    return (factor * blocks).astype(jnp.float32)


def draw_layer_inverse(key, part):
    return symmetric_blocks(jax.random.fold_in(key, 11), (ENERGIES, LAYERS), 1.0)


def draw_coupling(key, part):
    coupling_key = jax.random.fold_in(key, 14)
    spread = 1.36 * M ** (-0.5)
    values = jnp.clip(spread * jax.random.normal(coupling_key, (M, M), jnp.float32), -6.0 * spread, 6.0 * spread)
    return values.astype(jnp.float32)


def draw_lead_left(key, part):
    return symmetric_blocks(jax.random.fold_in(key, 12), (ENERGIES,), 0.5)


def draw_lead_right(key, part):
    return symmetric_blocks(jax.random.fold_in(key, 13), (ENERGIES,), 0.5)


def set_ends(drawn, rng, least, top_value):
    longest = drawn.shape.index(max(drawn.shape))
    spots = []
    for shift in (0, 1):
        where = [jax.random.randint(jax.random.fold_in(rng, axis), (), 0, length) for axis, length in enumerate(drawn.shape)]
        where[longest] = (where[longest] + shift) % drawn.shape[longest]
        spots.append(tuple(where))
    return drawn.at[spots[0]].set(least).at[spots[1]].set(top_value)


def shard_levels(key, shape, pieces, low, top_value):
    gain, own = 1.0, jax.random.fold_in(key, 6)
    for position, shards_of in pieces:
        steps = jnp.exp(jax.random.uniform(jax.random.fold_in(own, position), (shards_of,), jnp.float32, low / len(pieces), top_value / len(pieces)))
        gain = gain * jnp.repeat(steps, shape[position] // shards_of).reshape([-1 if axis == position else 1 for axis in range(len(shape))])
    return gain


def gaussian(key, shape, deviation, most, cuts=(), kind=jnp.bfloat16):
    array = jax.random.normal(key, shape, jnp.float32) * deviation
    if len(cuts) > 0:
        array = shard_levels(key, shape, cuts, -0.22, 0.18) * array
    return jnp.clip(array, min=-most, max=most).astype(kind)


def setup_inputs(seed: int = 0) -> dict:
    splits = jax.random.split(jax.random.key(seed), 10)
    return {
        "layer_inverse": draw_layer_inverse(jax.random.fold_in(splits[9], 71), 0),
        "coupling": draw_coupling(jax.random.fold_in(splits[9], 71), 0),
        "lead_left": draw_lead_left(jax.random.fold_in(splits[9], 71), 0),
        "lead_right": draw_lead_right(jax.random.fold_in(splits[9], 71), 0),
        "quad_weight": jnp.clip(jnp.exp(jax.random.uniform(splits[4], (ENERGIES,), jnp.float32, math.log(0.0015625), math.log(0.0625))), 0.0015625, 0.0625),
        "energy_slot": jax.random.permutation(splits[5], ENERGIES).astype(jnp.int32),
        "plane_of": set_ends(jax.random.randint(splits[6], (LAYERS,), 0, NX), jax.random.fold_in(splits[6], 1), 0, NX - 1).astype(jnp.int32),
        "doping": gaussian(splits[7], (NX, NY, NZ), 1.0, 6.0, ((0, 256),), jnp.float32),
        "screening": jnp.clip(0.25 + 1.75 * jax.random.uniform(splits[8], (NX, NY, NZ), jnp.float32) ** shard_levels(splits[8], (NX, NY, NZ), ((0, 256),), -0.2, 0.2), 0.25, 2.0),
    }


exact_mode = lax.Precision.HIGHEST


def matmul_hi(left_mat, right_mat):
    return jnp.matmul(left_mat, right_mat, precision=exact_mode)


def chain_diagonals(tmat, energy_item):
    inverse, left_lead, right_lead = energy_item
    forward = matmul_hi(inverse, tmat)
    backward = matmul_hi(inverse, tmat.T)

    def step_chain(state_mat, layer_pair):
        inv_layer, propagator = layer_pair
        following = inv_layer + matmul_hi(matmul_hi(propagator, state_mat), propagator.T)
        return following, state_mat

    _, left_in = lax.scan(step_chain, left_lead, (inverse, forward))
    _, right_in = lax.scan(step_chain, right_lead, (inverse, backward), reverse=True)
    self_energy = matmul_hi(matmul_hi(tmat, left_in), tmat.T) + matmul_hi(matmul_hi(tmat.T, right_in), tmat)
    dressed = matmul_hi(inverse, self_energy)
    return jnp.diagonal(inverse, axis1=1, axis2=2) + jnp.sum(dressed * jnp.swapaxes(inverse, 1, 2), axis=2)


def operate(values_in, screening):
    padded = jnp.pad(values_in, 1)
    beside = padded[2:, 1:-1, 1:-1] + padded[:-2, 1:-1, 1:-1]
    beside = beside + padded[1:-1, 2:, 1:-1] + padded[1:-1, :-2, 1:-1]
    beside = beside + padded[1:-1, 1:-1, 2:] + padded[1:-1, 1:-1, :-2]
    return (6.0 + screening) * values_in - beside


def reference(layer_inverse, coupling, lead_left, lead_right, quad_weight, energy_slot, plane_of, doping, screening):
    diagonals = lax.map(partial(chain_diagonals, coupling), (layer_inverse, lead_left, lead_right))
    weight = quad_weight[energy_slot]
    layer_density = jnp.sum(weight[:, None, None] * diagonals, axis=0)
    plane_ids = jnp.arange(NX, dtype=jnp.int32)
    onehot = (plane_of[None, :] == plane_ids[:, None]).astype(jnp.float32)
    plane_charge = jnp.dot(onehot, layer_density, precision=exact_mode).reshape(NX, ORB_Y, ORB_Z)
    charge = jnp.repeat(jnp.repeat(plane_charge, NY // ORB_Y, axis=1), NZ // ORB_Z, axis=2)
    source = charge - doping
    potential = jnp.zeros_like(source)
    residual, direction = source, source
    norm_now = jnp.sum(residual * residual)
    for iteration in range(CG_ITERS):
        applied = operate(direction, screening)
        step_size = norm_now / jnp.sum(direction * applied)
        potential = potential + step_size * direction
        residual = residual - step_size * applied
        norm_next = jnp.sum(residual * residual)
        direction = residual + (norm_next / norm_now) * direction
        norm_now = norm_next
    return layer_density, potential, residual
```

```python
import functools

import jax
import jax.numpy as jnp
from jax import lax
from jax.experimental import pallas as pl
from jax.experimental.pallas import tpu as pltpu
from jax.sharding import Mesh
from jax.sharding import PartitionSpec as P

LAYER = ("layer_0", "layer_1")
ENERGY_LAYER = ("energy_0", "energy_1", "energy_2", "layer_0", "layer_1")
DEEP = ("energy_2",)
ACROSS = ("energy_0", "energy_1", "layer_0", "layer_1")
ENERGY = ("energy_0", "energy_1", "energy_2")

F32, BF16 = jnp.float32, jnp.bfloat16
NN = (((1,), (0,)), ((), ()))
NT = (((1,), (1,)), ((), ()))
VMEM = pl.BlockSpec(memory_space=pltpu.VMEM)
SMEM = pl.BlockSpec(memory_space=pltpu.SMEM)
HALF = 128
PACKED = 2 * HALF + 8
SHIFT = 7.125


def halves(x):
    high = x.astype(BF16)
    return high, (x - high.astype(F32)).astype(BF16)


def product(a, b, dims):
    dot = functools.partial(lax.dot_general, dimension_numbers=dims, preferred_element_type=F32)
    return dot(a[0], b[0]) + (dot(a[0], b[1]) + dot(a[1], b[0]))


def square_iota(n):
    return (lax.broadcasted_iota(jnp.int32, (n, n), 0), lax.broadcasted_iota(jnp.int32, (n, n), 1))


def diagonal_row(x):
    rows, cols = square_iota(x.shape[0])
    return jnp.sum(jnp.where(rows == cols, x, 0.0), axis=0, keepdims=True)


def pack(out_ref, x):
    rows, cols = square_iota(HALF)
    low, high = x[:HALF, :HALF], x[HALF:, HALF:]
    out_ref[:HALF, :] = x[:HALF, HALF:]
    out_ref[HALF : 2 * HALF, :] = jnp.where(rows >= cols, low, high)
    out_ref[2 * HALF :, :] = jnp.broadcast_to(diagonal_row(high), (8, HALF))


def unpack(ref, out_ref):
    rows, cols = square_iota(HALF)
    off, both = ref[:HALF, :], ref[HALF : 2 * HALF, :]
    flipped = both.T
    out_ref[:HALF, :HALF] = jnp.where(rows >= cols, both, flipped)
    out_ref[:HALF, HALF:] = off
    out_ref[HALF:, :HALF] = off.T
    high = jnp.where(rows < cols, both, flipped)
    out_ref[HALF:, HALF:] = jnp.where(rows == cols, ref[2 * HALF : 2 * HALF + 1, :], high)


def chain_kernel(
    place, d_ref, t_ref, lead_ref, lead_r_ref,
    send_ref, base_ref, state_ref, map_h, map_l, kh_ref, kl_ref,
    ph, pw,
):
    layers = d_ref.shape[0]
    coupling = halves(t_ref[...])

    @pl.loop(0, layers)
    def _(layer):
        inverse = d_ref[layer]
        split = halves(inverse)
        for side, dims in ((0, NN), (1, NT)):
            high, low = halves(product(split, coupling, dims))
            ph[side, layer] = high
            pw[side, layer] = low
        base_ref[pl.ds(layer, 1), :] = -diagonal_row(inverse)

    rows, cols = square_iota(d_ref.shape[1])
    for side, first in ((0, 0), (1, layers - 1)):
        state_ref[side] = d_ref[first]
        base_ref[first : first + 1, :] += diagonal_row(d_ref[first])
        start = (ph[side, first].astype(F32) + pw[side, first].astype(F32)).T
        kh_ref[side, first], kl_ref[side, first] = halves(start)

    @pl.loop(1, layers)
    def _(step):
        for side in (0, 1):
            layer = step if side == 0 else layers - 1 - step
            before = step - 1 if side == 0 else layers - step
            move = (ph[side, layer], pw[side, layer])
            carried = product((kh_ref[side, before], kl_ref[side, before]), move, NT)
            kh_ref[side, layer], kl_ref[side, layer] = halves(carried)
            half_way = product(move, halves(state_ref[side]), NN)
            updated = d_ref[layer] + product(halves(half_way), move, NT)
            state_ref[side] = updated
            base_ref[pl.ds(layer, 1), :] += diagonal_row(updated)

    for side, last in ((0, layers - 1), (1, 0)):
        whole = (kh_ref[side, last].astype(F32) + kl_ref[side, last].astype(F32)).T
        map_h[side], map_l[side] = halves(whole)
    side = (place[0] >= 2).astype(jnp.int32)
    entering = jnp.where(place[0] >= 2, lead_r_ref[...], lead_ref[...])
    pack(send_ref, through(entering, side, state_ref, map_h, map_l))


def through(entering, side, state_ref, map_h, map_l):
    whole = (map_h[side], map_l[side])
    half_way = product(whole, halves(entering), NN)
    return state_ref[side] + product(halves(half_way), whole, NT)


def hop_kernel(right_at, place, received_ref, state_ref, map_h, map_l, send_ref, full):
    unpack(received_ref, full)
    side = (place[0] == right_at).astype(jnp.int32)
    pack(send_ref, through(full[...], side, state_ref, map_h, map_l))


def add_corrections(side, full, base_ref, kh_ref, kl_ref, out_ref):
    entering = halves(full[...])
    for layer in range(base_ref.shape[0]):
        high, low = kh_ref[side, layer], kl_ref[side, layer]
        moved = product(entering, (high, low), NN)
        carried = high.astype(F32) + low.astype(F32)
        row = jnp.sum(moved * carried, axis=0, keepdims=True)
        out_ref[layer : layer + 1, :] = base_ref[layer : layer + 1, :] + row


def first_kernel(place, received_ref, lead_ref, lead_r_ref, base_ref, kh_ref, kl_ref, out_ref, full):
    segment = place[0]

    @pl.when(segment == 0)
    def _():
        full[...] = lead_ref[...]

    @pl.when(segment == 3)
    def _():
        full[...] = lead_r_ref[...]

    @pl.when((segment == 1) | (segment == 2))
    def _():
        unpack(received_ref, full)

    side = (segment >= 2).astype(jnp.int32)
    add_corrections(side, full, base_ref, kh_ref, kl_ref, out_ref)


def second_kernel(
    place, slot, weights, third_ref, second_ref, base_ref, kh_ref, kl_ref, out_ref, full, rows_ref
):
    segment = place[0]

    @pl.when((segment == 0) | (segment == 3))
    def _():
        unpack(third_ref, full)

    @pl.when((segment == 1) | (segment == 2))
    def _():
        unpack(second_ref, full)

    side = (segment < 2).astype(jnp.int32)
    add_corrections(side, full, base_ref, kh_ref, kl_ref, rows_ref)
    weighted = rows_ref[...] * weights[slot[0]]
    for peer in range(out_ref.shape[0]):
        out_ref[peer] = weighted


def fan_kernel(pieces_ref, out_ref):
    total = pieces_ref[0]
    for peer in range(1, pieces_ref.shape[0]):
        total = total + pieces_ref[peer]
    for peer in range(out_ref.shape[0]):
        out_ref[peer] = total


def krylov_kernel(
    place, plane_of, pieces_ref, doping_ref, screening_ref, below_ref, above_ref,
    own_rows_ref, basis_ref, sums_ref, src, one, two, density_ref,
):
    slab, last_slab = place[1], place[2]
    layers = pieces_ref.shape[1]
    segments = plane_of.shape[0] // layers
    for segment in range(segments):
        rows = pieces_ref[segment]
        for piece in range(segments + segment, pieces_ref.shape[0], segments):
            rows = rows + pieces_ref[piece]
        density_ref[segment * layers : (segment + 1) * layers, :] = rows
    own_rows_ref[...] = density_ref[pl.ds(pl.multiple_of(place[0] * layers, layers), layers), :]
    own = doping_ref.shape[0]
    depth = 3
    y_cells, z_cells = doping_ref.shape[1:]
    rows, cols = square_iota(y_cells)
    orbitals = density_ref.shape[1]
    for i in range(own + 2 * depth):
        if i < depth:
            src[i] = -below_ref[i]
        elif i < depth + own:
            src[i] = -doping_ref[i - depth]
        else:
            src[i] = -above_ref[i - depth - own]

    first_plane = slab * own - depth

    @pl.loop(0, plane_of.shape[0])
    def _(layer):
        at = plane_of[layer] - first_plane

        @pl.when((at >= 0) & (at < own + 2 * depth))
        def _():
            width = 16
            row = jnp.broadcast_to(density_ref[pl.ds(layer, 1), :], (y_cells, orbitals))
            yy = lax.broadcasted_iota(jnp.int32, (y_cells, orbitals), 0)
            mm = lax.broadcasted_iota(jnp.int32, (y_cells, orbitals), 1)
            spread = jnp.where(mm // width == yy // (y_cells // width), row, 0.0)
            zz = lax.broadcasted_iota(jnp.int32, (orbitals, z_cells), 1)
            mz = lax.broadcasted_iota(jnp.int32, (orbitals, z_cells), 0)
            pick = (mz % width == zz // (z_cells // width)).astype(F32).astype(BF16)
            high, low = halves(spread)
            lowest = (spread - high.astype(F32) - low.astype(F32)).astype(BF16)
            dot = functools.partial(
                lax.dot_general, dimension_numbers=NN, preferred_element_type=F32
            )
            src[at] = src[at] + (dot(high, pick) + (dot(low, pick) + dot(lowest, pick)))

    def screen(i):
        if i < depth:
            return below_ref[i + 2]
        if i < depth + own:
            return screening_ref[i - depth]
        return above_ref[i - own]

    def shifted_operator(ref, i):
        plane = ref[i]
        beside = ref[i - 1] + ref[i + 1]
        beside = beside + jnp.where(rows == 0, 0.0, pltpu.roll(plane, 1, 0))
        beside = beside + jnp.where(rows == y_cells - 1, 0.0, pltpu.roll(plane, y_cells - 1, 0))
        beside = beside + jnp.where(cols == 0, 0.0, pltpu.roll(plane, 1, 1))
        beside = beside + jnp.where(cols == z_cells - 1, 0.0, pltpu.roll(plane, z_cells - 1, 1))
        return (screen(i) + (6.0 - SHIFT)) * plane - beside

    inside_low = jnp.where(slab == 0, 0.0, 1.0)
    inside_high = jnp.where(slab == last_slab, 0.0, 1.0)

    def masked(i, plane):
        if i < depth:
            return plane * inside_low
        if i >= depth + own:
            return plane * inside_high
        return plane

    for i in range(1, own + 2 * depth - 1):
        one[i] = masked(i, shifted_operator(src, i))
    for i in range(2, own + 2 * depth - 2):
        two[i] = masked(i, shifted_operator(one, i))
    totals = [jnp.zeros((y_cells, z_cells), F32) for _ in range(6)]
    for i in range(depth, depth + own):
        three = shifted_operator(two, i)
        v = (src[i], one[i], two[i], three)
        for k in range(4):
            basis_ref[k, i - depth] = v[k]
        for k in range(6):
            totals[k] = totals[k] + v[k // 2] * v[k - k // 2]
    lane = lax.broadcasted_iota(jnp.int32, (1, z_cells), 1)
    out = jnp.zeros((1, z_cells), F32)
    for k in range(6):
        total = jnp.sum(jnp.sum(totals[k], axis=0, keepdims=True), axis=1, keepdims=True)
        out = out + jnp.where(lane == k, total, 0.0)
    for peer in range(sums_ref.shape[0]):
        sums_ref[peer] = out


def finish_kernel(sums_ref, basis_ref, potential_ref, residual_ref):
    total = jnp.sum(sums_ref[...], axis=0)
    lane = lax.broadcasted_iota(jnp.int32, total.shape, 1)
    m = [jnp.sum(jnp.where(lane == k, total, 0.0), axis=1, keepdims=True) for k in range(6)]

    def inner(a, b):
        terms = [x * y * m[i + j] for i, x in enumerate(a) for j, y in enumerate(b)]
        return functools.reduce(lambda p, q: p + q, terms)

    def applied(c):
        moved = [SHIFT * x for x in c] + [c[-1]]
        for i in range(len(c) - 1):
            moved[i + 1] = moved[i + 1] + c[i]
        return moved

    def plus(a, scale, b):
        n = max(len(a), len(b))
        a = list(a) + [None] * (n - len(a))
        b = list(b) + [None] * (n - len(b))
        return [
            x if y is None else (scale * y if x is None else x + scale * y) for x, y in zip(a, b)
        ]

    unit = jnp.ones_like(m[0])
    residual = [unit]
    direction = [unit]
    potential = []
    norm = m[0]
    for iteration in range(3):
        image = applied(direction)
        step = norm / inner(direction, image)
        potential = plus(potential, step, direction)
        residual = plus(residual, -step, image)
        if iteration < 2:
            following = inner(residual, residual)
            direction = plus(residual, following / norm, direction)
            norm = following
    for i in range(potential_ref.shape[0]):
        v = [basis_ref[k, i] for k in range(4)]
        potential_ref[i] = potential[0] * v[0] + potential[1] * v[1] + potential[2] * v[2]
        residual_ref[i] = (
            residual[0] * v[0] + residual[1] * v[1] + residual[2] * v[2] + residual[3] * v[3]
        )


def call(kernel, out_shape, in_specs, scratch=(), flops=0, out_specs=None, name=None):
    return pl.pallas_call(
        kernel,
        out_shape=out_shape,
        in_specs=in_specs,
        out_specs=jax.tree.map(lambda _: VMEM, out_shape) if out_specs is None else out_specs,
        scratch_shapes=list(scratch),
        name=name,
        cost_estimate=pl.CostEstimate(flops=flops, bytes_accessed=0, transcendentals=0),
        compiler_params=pltpu.CompilerParams(vmem_limit_bytes=40 * 2**20),
    )


def shape(*dims, dtype=F32):
    return jax.ShapeDtypeStruct(dims, dtype)


def exchange(copies, axis):
    return lax.all_to_all(copies, axis, 0, 0, tiled=True)


def body(
    layer_inverse, coupling, lead_left, lead_right, quad_weight, energy_slot, plane_of, doping, screening
):
    inverse, left, right = layer_inverse[0], lead_left[0], lead_right[0]
    layers, size = inverse.shape[0], inverse.shape[1]
    slab = lax.axis_index(ENERGY_LAYER)
    slabs = lax.axis_size(ENERGY_LAYER)
    place = jnp.stack([lax.axis_index(LAYER), slab, jnp.int32(slabs - 1)]).astype(jnp.int32)
    own, ny, nz = doping.shape

    up = [(i, i + 1) for i in range(slabs - 1)]
    down = [(i + 1, i) for i in range(slabs - 1)]
    below = lax.ppermute(jnp.concatenate([doping[own - 3 :], screening[own - 2 :]]), ENERGY_LAYER, up)
    above = lax.ppermute(jnp.concatenate([doping[:3], screening[:2]]), ENERGY_LAYER, down)

    send, base, state, map_h, map_l, kh, kl = call(
        chain_kernel,
        (
            shape(PACKED, HALF), shape(layers, size), shape(2, size, size),
            shape(2, size, size, dtype=BF16), shape(2, size, size, dtype=BF16),
            shape(2, layers, size, size, dtype=BF16), shape(2, layers, size, size, dtype=BF16),
        ),
        [SMEM, VMEM, VMEM, VMEM, VMEM],
        [pltpu.VMEM((2, layers, size, size), BF16)] * 2,
        flops=10**7, name="chain",
    )(place, inverse, coupling, left, right)

    def hop(received, right_at):
        return call(
            functools.partial(hop_kernel, right_at), shape(PACKED, HALF),
            [SMEM, VMEM, VMEM, VMEM, VMEM], [pltpu.VMEM((size, size), F32)],
            flops=10**6, name=f"hop_{right_at}",
        )(place, received, state, map_h, map_l)

    first = lax.ppermute(send, LAYER, [(0, 1), (3, 2)])
    second = lax.ppermute(hop(first, 2), LAYER, [(1, 2), (2, 1)])
    once = call(
        first_kernel, shape(layers, size), [SMEM] + [VMEM] * 6, [pltpu.VMEM((size, size), F32)],
        flops=10**7, name="first",
    )(place, first, left, right, base, kh, kl)
    third = lax.ppermute(hop(second, 1), LAYER, [(2, 3), (1, 0)])
    partial = call(
        second_kernel, shape(lax.axis_size(DEEP), layers, size), [SMEM] * 3 + [VMEM] * 5,
        [pltpu.VMEM((size, size), F32), pltpu.VMEM((layers, size), F32)],
        flops=10**7, name="second",
    )(place, energy_slot, quad_weight, third, second, once, kh, kl)
    along_z = exchange(partial, DEEP)
    fanned = call(
        fan_kernel, shape(lax.axis_size(ACROSS), layers, size), [VMEM], flops=10**6, name="fan"
    )(along_z)
    pieces = exchange(fanned, ACROSS)

    own_rows, basis, sums = call(
        krylov_kernel,
        (shape(layers, size), shape(4, own, ny, nz), shape(slabs, 1, nz)),
        [SMEM, SMEM] + [VMEM] * 5,
        [pltpu.VMEM((own + 6, ny, nz), F32)] * 3 + [pltpu.VMEM((plane_of.shape[0], size), F32)],
        flops=10**6, name="krylov",
    )(place, plane_of, pieces, doping, screening, below, above)
    all_sums = exchange(sums, ENERGY_LAYER)
    potential, residual = call(
        finish_kernel, (shape(own, ny, nz), shape(own, ny, nz)), [VMEM] * 2,
        flops=10**6, name="finish",
    )(all_sums, basis)
    return own_rows, potential, residual


def solution(mesh):
    split = Mesh(
        mesh.devices.reshape(4, 2, 8, 2, 2),
        ("energy_0", "energy_1", "energy_2", "layer_0", "layer_1"),
    )
    in_specs = (
        P(ENERGY, LAYER, None, None),
        P(),
        P(ENERGY, None, None),
        P(ENERGY, None, None),
        P(),
        P(ENERGY),
        P(),
        P(ENERGY_LAYER, None, None),
        P(ENERGY_LAYER, None, None),
    )
    out_specs = (P(LAYER, None), P(ENERGY_LAYER, None, None), P(ENERGY_LAYER, None, None))
    return jax.shard_map(body, mesh=split, in_specs=in_specs, out_specs=out_specs, check_vma=False)
```

```python
import functools

import jax
import jax.numpy as jnp
from jax import lax
from jax.experimental import pallas as pl
from jax.experimental.pallas import tpu as pltpu
from jax.sharding import Mesh
from jax.sharding import PartitionSpec as P

LAYER = ("layer_0", "layer_1")
ENERGY_LAYER = ("energy_0", "energy_1", "energy_2", "layer_0", "layer_1")
DEEP = ("energy_2",)
ACROSS = ("energy_0", "energy_1", "layer_0", "layer_1")
ENERGY = ("energy_0", "energy_1", "energy_2")

F32, BF16 = jnp.float32, jnp.bfloat16
NN = (((1,), (0,)), ((), ()))
NT = (((1,), (1,)), ((), ()))
VMEM = pl.BlockSpec(memory_space=pltpu.VMEM)
HBM = pl.BlockSpec(memory_space=pltpu.HBM)
SMEM = pl.BlockSpec(memory_space=pltpu.SMEM)
HALF = 128
PACKED = 2 * HALF + 8
SHIFT = 7.125


def halves(x):
    high = x.astype(BF16)
    return high, (x - high.astype(F32)).astype(BF16)


def product(a, b, dims):
    dot = functools.partial(lax.dot_general, dimension_numbers=dims, preferred_element_type=F32)
    return dot(a[0], b[0]) + (dot(a[0], b[1]) + dot(a[1], b[0]))


def square_iota(n):
    return (lax.broadcasted_iota(jnp.int32, (n, n), 0), lax.broadcasted_iota(jnp.int32, (n, n), 1))


def diagonal_row(x):
    rows, cols = square_iota(x.shape[0])
    return jnp.sum(jnp.where(rows == cols, x, 0.0), axis=0, keepdims=True)


def pack(out_ref, x):
    rows, cols = square_iota(HALF)
    low, high = x[:HALF, :HALF], x[HALF:, HALF:]
    out_ref[:HALF, :] = x[:HALF, HALF:]
    out_ref[HALF : 2 * HALF, :] = jnp.where(rows >= cols, low, high)
    out_ref[2 * HALF :, :] = jnp.broadcast_to(diagonal_row(high), (8, HALF))


def unpack(ref, out_ref):
    rows, cols = square_iota(HALF)
    off, both = ref[:HALF, :], ref[HALF : 2 * HALF, :]
    flipped = both.T
    out_ref[:HALF, :HALF] = jnp.where(rows >= cols, both, flipped)
    out_ref[:HALF, HALF:] = off
    out_ref[HALF:, :HALF] = off.T
    high = jnp.where(rows < cols, both, flipped)
    out_ref[HALF:, HALF:] = jnp.where(rows == cols, ref[2 * HALF : 2 * HALF + 1, :], high)


def chain_kernel(
    place, d_hbm, t_hbm, lead_hbm, lead_r_hbm,
    send_ref, base_ref, state_ref, map_h, map_l, kh_ref, kl_ref,
    d_ref, t_ref, lead, ph, pw, arrived,
):
    layers = d_ref.shape[0]
    copies = [pltpu.make_async_copy(t_hbm, t_ref, arrived.at[0])]
    for layer in range(layers):
        copies.append(
            pltpu.make_async_copy(d_hbm.at[layer], d_ref.at[layer], arrived.at[1 + layer])
        )
    for copy in copies:
        copy.start()

    @pl.when(place[0] < 2)
    def _():
        pltpu.make_async_copy(lead_hbm, lead, arrived.at[1 + layers]).start()

    @pl.when(place[0] >= 2)
    def _():
        pltpu.make_async_copy(lead_r_hbm, lead, arrived.at[1 + layers]).start()

    copies[0].wait()
    coupling = halves(t_ref[...])
    for layer in range(layers):
        copies[1 + layer].wait()
        inverse = d_ref[layer]
        split = halves(inverse)
        for side, dims in ((0, NN), (1, NT)):
            high, low = halves(product(split, coupling, dims))
            ph[side, layer] = high
            pw[side, layer] = low
        base_ref[layer : layer + 1, :] = -diagonal_row(inverse)

    rows, cols = square_iota(d_ref.shape[1])
    for side, first in ((0, 0), (1, layers - 1)):
        state_ref[side] = d_ref[first]
        base_ref[first : first + 1, :] += diagonal_row(d_ref[first])
        start = (ph[side, first].astype(F32) + pw[side, first].astype(F32)).T
        kh_ref[side, first], kl_ref[side, first] = halves(start)

    @pl.loop(1, layers)
    def _(step):
        for side in (0, 1):
            layer = step if side == 0 else layers - 1 - step
            before = step - 1 if side == 0 else layers - step
            move = (ph[side, layer], pw[side, layer])
            carried = product((kh_ref[side, before], kl_ref[side, before]), move, NT)
            kh_ref[side, layer], kl_ref[side, layer] = halves(carried)
            half_way = product(move, halves(state_ref[side]), NN)
            updated = d_ref[layer] + product(halves(half_way), move, NT)
            state_ref[side] = updated
            base_ref[pl.ds(layer, 1), :] += diagonal_row(updated)

    for side, last in ((0, layers - 1), (1, 0)):
        whole = (kh_ref[side, last].astype(F32) + kl_ref[side, last].astype(F32)).T
        map_h[side], map_l[side] = halves(whole)
    side = (place[0] >= 2).astype(jnp.int32)
    pltpu.make_async_copy(lead_hbm, lead, arrived.at[1 + layers]).wait()
    pack(send_ref, through(lead[...], side, state_ref, map_h, map_l))


def through(entering, side, state_ref, map_h, map_l):
    whole = (map_h[side], map_l[side])
    half_way = product(whole, halves(entering), NN)
    return state_ref[side] + product(halves(half_way), whole, NT)


def hop_kernel(right_at, place, received_ref, state_ref, map_h, map_l, send_ref, full):
    unpack(received_ref, full)
    side = (place[0] == right_at).astype(jnp.int32)
    pack(send_ref, through(full[...], side, state_ref, map_h, map_l))


def add_corrections(side, full, base_ref, kh_ref, kl_ref, out_ref):
    entering = halves(full[...])
    for layer in range(base_ref.shape[0]):
        high, low = kh_ref[side, layer], kl_ref[side, layer]
        moved = product(entering, (high, low), NN)
        carried = high.astype(F32) + low.astype(F32)
        row = jnp.sum(moved * carried, axis=0, keepdims=True)
        out_ref[layer : layer + 1, :] = base_ref[layer : layer + 1, :] + row


def first_kernel(
    place, received_ref, lead_hbm, lead_r_hbm, base_ref, kh_ref, kl_ref, out_ref, full
):
    segment = place[0]

    @pl.when(segment == 0)
    def _():
        pltpu.sync_copy(lead_hbm, full)

    @pl.when(segment == 3)
    def _():
        pltpu.sync_copy(lead_r_hbm, full)

    @pl.when((segment == 1) | (segment == 2))
    def _():
        unpack(received_ref, full)

    side = (segment >= 2).astype(jnp.int32)
    add_corrections(side, full, base_ref, kh_ref, kl_ref, out_ref)


def second_kernel(
    place, slot, weights, third_ref, second_ref, base_ref, kh_ref, kl_ref, out_ref, full, rows_ref
):
    segment = place[0]

    @pl.when((segment == 0) | (segment == 3))
    def _():
        unpack(third_ref, full)

    @pl.when((segment == 1) | (segment == 2))
    def _():
        unpack(second_ref, full)

    side = (segment < 2).astype(jnp.int32)
    add_corrections(side, full, base_ref, kh_ref, kl_ref, rows_ref)
    weighted = rows_ref[...] * weights[slot[0]]
    for peer in range(out_ref.shape[0]):
        out_ref[peer] = weighted


def fan_kernel(pieces_ref, out_ref):
    total = pieces_ref[0]
    for peer in range(1, pieces_ref.shape[0]):
        total = total + pieces_ref[peer]
    for peer in range(out_ref.shape[0]):
        out_ref[peer] = total


DEPTH = 3


def grid_kernel(
    place, doping_hbm, screening_hbm, below_ref, above_ref, field_ref, screen_ref, arrived
):
    own, planes = doping_hbm.shape[0], field_ref.shape[0]
    copies = [
        pltpu.make_async_copy(doping_hbm, field_ref.at[pl.ds(DEPTH, own)], arrived.at[0]),
        pltpu.make_async_copy(screening_hbm, screen_ref.at[pl.ds(DEPTH, own)], arrived.at[1]),
    ]
    for copy in copies:
        copy.start()
    inside_low = jnp.where(place[1] == 0, 0.0, 1.0)
    inside_high = jnp.where(place[1] == place[2], 0.0, 1.0)
    for i in range(DEPTH):
        field_ref[i] = below_ref[i] * -inside_low
        field_ref[planes - DEPTH + i] = above_ref[i] * -inside_high
    for i in range(DEPTH - 1):
        screen_ref[i + 1] = below_ref[DEPTH + i]
        screen_ref[planes - DEPTH + i] = above_ref[DEPTH + i]
    for copy in copies:
        copy.wait()
    for i in range(DEPTH, DEPTH + own):
        field_ref[i] = -field_ref[i]


def krylov_kernel(
    place, plane_of, pieces_ref, field_ref, screen_ref,
    own_rows_ref, basis_ref, sums_ref, src, one, two, density_ref,
):
    slab, last_slab = place[1], place[2]
    layers = pieces_ref.shape[1]
    segments = plane_of.shape[0] // layers
    for segment in range(segments):
        rows = pieces_ref[segment]
        for piece in range(segments + segment, pieces_ref.shape[0], segments):
            rows = rows + pieces_ref[piece]
        density_ref[segment * layers : (segment + 1) * layers, :] = rows
    own_rows_ref[...] = density_ref[pl.ds(pl.multiple_of(place[0] * layers, layers), layers), :]
    depth, own = DEPTH, basis_ref.shape[1]
    y_cells, z_cells = field_ref.shape[1:]
    rows, cols = square_iota(y_cells)
    orbitals = density_ref.shape[1]
    src[...] = field_ref[...]
    first_plane = slab * own - depth

    @pl.loop(0, plane_of.shape[0])
    def _(layer):
        at = plane_of[layer] - first_plane

        @pl.when((at >= 0) & (at < own + 2 * depth))
        def _():
            width = 16
            row = jnp.broadcast_to(density_ref[pl.ds(layer, 1), :], (y_cells, orbitals))
            yy = lax.broadcasted_iota(jnp.int32, (y_cells, orbitals), 0)
            mm = lax.broadcasted_iota(jnp.int32, (y_cells, orbitals), 1)
            spread = jnp.where(mm // width == yy // (y_cells // width), row, 0.0)
            zz = lax.broadcasted_iota(jnp.int32, (orbitals, z_cells), 1)
            mz = lax.broadcasted_iota(jnp.int32, (orbitals, z_cells), 0)
            pick = (mz % width == zz // (z_cells // width)).astype(F32).astype(BF16)
            high, low = halves(spread)
            lowest = (spread - high.astype(F32) - low.astype(F32)).astype(BF16)
            dot = functools.partial(
                lax.dot_general, dimension_numbers=NN, preferred_element_type=F32
            )
            src[at] = src[at] + (dot(high, pick) + (dot(low, pick) + dot(lowest, pick)))

    def shifted_operator(ref, i):
        plane = ref[i]
        beside = ref[i - 1] + ref[i + 1]
        beside = beside + jnp.where(rows == 0, 0.0, pltpu.roll(plane, 1, 0))
        beside = beside + jnp.where(rows == y_cells - 1, 0.0, pltpu.roll(plane, y_cells - 1, 0))
        beside = beside + jnp.where(cols == 0, 0.0, pltpu.roll(plane, 1, 1))
        beside = beside + jnp.where(cols == z_cells - 1, 0.0, pltpu.roll(plane, z_cells - 1, 1))
        return (screen_ref[i] + (6.0 - SHIFT)) * plane - beside

    inside_low = jnp.where(slab == 0, 0.0, 1.0)
    inside_high = jnp.where(slab == last_slab, 0.0, 1.0)

    def masked(i, plane):
        if i < depth:
            return plane * inside_low
        if i >= depth + own:
            return plane * inside_high
        return plane

    for i in range(1, own + 2 * depth - 1):
        one[i] = masked(i, shifted_operator(src, i))
    for i in range(2, own + 2 * depth - 2):
        two[i] = masked(i, shifted_operator(one, i))
    totals = [jnp.zeros((y_cells, z_cells), F32) for _ in range(6)]
    for i in range(depth, depth + own):
        three = shifted_operator(two, i)
        v = (src[i], one[i], two[i], three)
        for k in range(4):
            basis_ref[k, i - depth] = v[k]
        for k in range(6):
            totals[k] = totals[k] + v[k // 2] * v[k - k // 2]
    lane = lax.broadcasted_iota(jnp.int32, (1, z_cells), 1)
    out = jnp.zeros((1, z_cells), F32)
    for k in range(6):
        total = jnp.sum(jnp.sum(totals[k], axis=0, keepdims=True), axis=1, keepdims=True)
        out = out + jnp.where(lane == k, total, 0.0)
    for peer in range(sums_ref.shape[0]):
        sums_ref[peer] = out


def finish_kernel(sums_ref, basis_ref, potential_ref, residual_ref):
    total = jnp.sum(sums_ref[...], axis=0)
    lane = lax.broadcasted_iota(jnp.int32, total.shape, 1)
    m = [jnp.sum(jnp.where(lane == k, total, 0.0), axis=1, keepdims=True) for k in range(6)]

    def inner(a, b):
        terms = [x * y * m[i + j] for i, x in enumerate(a) for j, y in enumerate(b)]
        return functools.reduce(lambda p, q: p + q, terms)

    def applied(c):
        moved = [SHIFT * x for x in c] + [c[-1]]
        for i in range(len(c) - 1):
            moved[i + 1] = moved[i + 1] + c[i]
        return moved

    def plus(a, scale, b):
        n = max(len(a), len(b))
        a = list(a) + [None] * (n - len(a))
        b = list(b) + [None] * (n - len(b))
        return [
            x if y is None else (scale * y if x is None else x + scale * y) for x, y in zip(a, b)
        ]

    unit = jnp.ones_like(m[0])
    residual = [unit]
    direction = [unit]
    potential = []
    norm = m[0]
    for iteration in range(3):
        image = applied(direction)
        step = norm / inner(direction, image)
        potential = plus(potential, step, direction)
        residual = plus(residual, -step, image)
        if iteration < 2:
            following = inner(residual, residual)
            direction = plus(residual, following / norm, direction)
            norm = following
    for i in range(potential_ref.shape[0]):
        v = [basis_ref[k, i] for k in range(4)]
        potential_ref[i] = potential[0] * v[0] + potential[1] * v[1] + potential[2] * v[2]
        residual_ref[i] = (
            residual[0] * v[0] + residual[1] * v[1] + residual[2] * v[2] + residual[3] * v[3]
        )


def call(kernel, out_shape, in_specs, scratch=(), flops=0, out_specs=None, name=None):
    return pl.pallas_call(
        kernel,
        out_shape=out_shape,
        in_specs=in_specs,
        out_specs=jax.tree.map(lambda _: VMEM, out_shape) if out_specs is None else out_specs,
        scratch_shapes=list(scratch),
        name=name,
        cost_estimate=pl.CostEstimate(flops=flops, bytes_accessed=0, transcendentals=0),
        compiler_params=pltpu.CompilerParams(vmem_limit_bytes=40 * 2**20),
    )


def shape(*dims, dtype=F32):
    return jax.ShapeDtypeStruct(dims, dtype)


def exchange(copies, axis):
    return lax.all_to_all(copies, axis, 0, 0, tiled=True)


def body(
    layer_inverse, coupling, lead_left, lead_right, quad_weight, energy_slot, plane_of, doping, screening
):
    inverse, left, right = layer_inverse[0], lead_left[0], lead_right[0]
    layers, size = inverse.shape[0], inverse.shape[1]
    slab = lax.axis_index(ENERGY_LAYER)
    slabs = lax.axis_size(ENERGY_LAYER)
    place = jnp.stack([lax.axis_index(LAYER), slab, jnp.int32(slabs - 1)]).astype(jnp.int32)
    own, ny, nz = doping.shape

    up = [(i, (i + 1) % slabs) for i in range(slabs)]
    down = [(j, i) for i, j in up]
    with jax.named_scope("halo_below"):
        edge = jnp.concatenate([doping[own - 3 :], screening[own - 2 :]])
        below = lax.ppermute(edge, ENERGY_LAYER, up)
    with jax.named_scope("halo_above"):
        edge = jnp.concatenate([doping[:3], screening[:2]])
        above = lax.ppermute(edge, ENERGY_LAYER, down)

    send, base, state, map_h, map_l, kh, kl = call(
        chain_kernel,
        (
            shape(PACKED, HALF), shape(layers, size), shape(2, size, size),
            shape(2, size, size, dtype=BF16), shape(2, size, size, dtype=BF16),
            shape(2, layers, size, size, dtype=BF16), shape(2, layers, size, size, dtype=BF16),
        ),
        [SMEM, HBM, HBM, HBM, HBM],
        [
            pltpu.VMEM((layers, size, size), F32), pltpu.VMEM((size, size), F32),
            pltpu.VMEM((size, size), F32),
            *[pltpu.VMEM((2, layers, size, size), BF16)] * 2,
            pltpu.SemaphoreType.DMA((layers + 2,)),
        ],
        flops=5 * 10**9, name="chain",
    )(place, inverse, coupling, left, right)

    def hop(received, right_at):
        return call(
            functools.partial(hop_kernel, right_at), shape(PACKED, HALF),
            [SMEM, VMEM, VMEM, VMEM, VMEM], [pltpu.VMEM((size, size), F32)],
            flops=2 * 10**8, name=f"hop_{right_at}",
        )(place, received, state, map_h, map_l)

    swap = [(0, 1), (1, 0), (2, 3), (3, 2)]
    send, below, above = lax.optimization_barrier((send, below, above))
    first = lax.ppermute(send, LAYER, swap)
    with jax.named_scope("middle"):
        second = lax.ppermute(hop(first, 2), LAYER, [(0, 0), (1, 2), (2, 1), (3, 3)])
    field, screen = call(
        grid_kernel, (shape(own + 6, ny, nz), shape(own + 6, ny, nz)),
        [SMEM, HBM, HBM, VMEM, VMEM], [pltpu.SemaphoreType.DMA((2,))],
        flops=2 * 10**8, name="grid",
    )(place, doping, screening, below, above)
    once = call(
        first_kernel, shape(layers, size), [SMEM, VMEM, HBM, HBM, VMEM, VMEM, VMEM],
        [pltpu.VMEM((size, size), F32)],
        flops=5 * 10**8, name="first",
    )(place, first, left, right, base, kh, kl)
    second, once, field, screen = lax.optimization_barrier((second, once, field, screen))
    third = lax.ppermute(hop(second, 1), LAYER, swap)
    partial = call(
        second_kernel, shape(lax.axis_size(DEEP), layers, size), [SMEM] * 3 + [VMEM] * 5,
        [pltpu.VMEM((size, size), F32), pltpu.VMEM((layers, size), F32)],
        flops=5 * 10**8, name="second",
    )(place, energy_slot, quad_weight, third, second, once, kh, kl)
    along_z = exchange(partial, DEEP)
    fanned = call(
        fan_kernel, shape(lax.axis_size(ACROSS), layers, size), [VMEM], flops=10**6, name="fan"
    )(along_z)
    pieces = exchange(fanned, ACROSS)

    own_rows, basis, sums = call(
        krylov_kernel,
        (shape(layers, size), shape(4, own, ny, nz), shape(slabs, 1, nz)),
        [SMEM, SMEM] + [VMEM] * 3,
        [pltpu.VMEM((own + 6, ny, nz), F32)] * 3 + [pltpu.VMEM((plane_of.shape[0], size), F32)],
        flops=10**6, name="krylov",
    )(place, plane_of, pieces, field, screen)
    all_sums = exchange(sums, ENERGY_LAYER)
    potential, residual = call(
        finish_kernel, (shape(own, ny, nz), shape(own, ny, nz)), [VMEM] * 2,
        flops=10**6, name="finish",
    )(all_sums, basis)
    return own_rows, potential, residual


def solution(mesh):
    split = Mesh(
        mesh.devices.reshape(4, 2, 8, 2, 2),
        ("energy_0", "energy_1", "energy_2", "layer_0", "layer_1"),
    )
    in_specs = (
        P(ENERGY, LAYER, None, None),
        P(),
        P(ENERGY, None, None),
        P(ENERGY, None, None),
        P(),
        P(ENERGY),
        P(),
        P(ENERGY_LAYER, None, None),
        P(ENERGY_LAYER, None, None),
    )
    out_specs = (P(LAYER, None), P(ENERGY_LAYER, None, None), P(ENERGY_LAYER, None, None))
    return jax.shard_map(body, mesh=split, in_specs=in_specs, out_specs=out_specs, check_vma=False)
```

```python
import functools

import jax
import jax.numpy as jnp
from jax import lax
from jax.experimental import pallas as pl
from jax.experimental.pallas import tpu as pltpu
from jax.sharding import Mesh
from jax.sharding import PartitionSpec as P

LAYER = ("layer_0", "layer_1")
ENERGY_LAYER = ("energy_0", "energy_1", "energy_2", "layer_0", "layer_1")
DEEP = ("energy_2",)
ACROSS = ("energy_0", "energy_1", "layer_0", "layer_1")
ENERGY = ("energy_0", "energy_1", "energy_2")

F32, BF16 = jnp.float32, jnp.bfloat16
NN = (((1,), (0,)), ((), ()))
NT = (((1,), (1,)), ((), ()))
VMEM = pl.BlockSpec(memory_space=pltpu.VMEM)
HBM = pl.BlockSpec(memory_space=pltpu.HBM)
SMEM = pl.BlockSpec(memory_space=pltpu.SMEM)
HALF = 128
PACKED = 2 * HALF + 8
SHIFT = 7.125


def halves(x):
    high = x.astype(BF16)
    return high, (x - high.astype(F32)).astype(BF16)


def product(a, b, dims):
    dot = functools.partial(lax.dot_general, dimension_numbers=dims, preferred_element_type=F32)
    return dot(a[0], b[0]) + (dot(a[0], b[1]) + dot(a[1], b[0]))


def square_iota(n):
    return (lax.broadcasted_iota(jnp.int32, (n, n), 0), lax.broadcasted_iota(jnp.int32, (n, n), 1))


def diagonal_row(x):
    rows, cols = square_iota(x.shape[0])
    return jnp.sum(jnp.where(rows == cols, x, 0.0), axis=0, keepdims=True)


def pack(out_ref, x):
    rows, cols = square_iota(HALF)
    low, high = x[:HALF, :HALF], x[HALF:, HALF:]
    out_ref[:HALF, :] = x[:HALF, HALF:]
    out_ref[HALF : 2 * HALF, :] = jnp.where(rows >= cols, low, high)
    out_ref[2 * HALF :, :] = jnp.broadcast_to(diagonal_row(high), (8, HALF))


def unpack(ref, out_ref):
    rows, cols = square_iota(HALF)
    off, both = ref[:HALF, :], ref[HALF : 2 * HALF, :]
    flipped = both.T
    out_ref[:HALF, :HALF] = jnp.where(rows >= cols, both, flipped)
    out_ref[:HALF, HALF:] = off
    out_ref[HALF:, :HALF] = off.T
    high = jnp.where(rows < cols, both, flipped)
    out_ref[HALF:, HALF:] = jnp.where(rows == cols, ref[2 * HALF : 2 * HALF + 1, :], high)


def chain_kernel(
    place, d_hbm, t_hbm, lead_hbm, lead_r_hbm,
    send_ref, base_ref, state_ref, map_h, map_l, kh_ref, kl_ref,
    d_ref, t_ref, lead, ph, pw, arrived,
):
    layers = d_ref.shape[0]
    order = [layer for pair in zip(range(layers), reversed(range(layers))) for layer in pair]
    copies = [pltpu.make_async_copy(t_hbm, t_ref, arrived.at[layers])]
    for layer in order[:layers]:
        copies.append(pltpu.make_async_copy(d_hbm.at[layer], d_ref.at[layer], arrived.at[layer]))
    for copy in copies:
        copy.start()

    @pl.when(place[0] < 2)
    def _():
        pltpu.make_async_copy(lead_hbm, lead, arrived.at[1 + layers]).start()

    @pl.when(place[0] >= 2)
    def _():
        pltpu.make_async_copy(lead_r_hbm, lead, arrived.at[1 + layers]).start()

    for copy in copies[:3]:
        copy.wait()
    coupling = halves(t_ref[...])
    seen = set()
    for step in range(layers):
        if step == 1:
            for copy in copies[3:]:
                copy.wait()
        for side, dims in ((0, NN), (1, NT)):
            layer = step if side == 0 else layers - 1 - step
            before = step - 1 if side == 0 else layers - step
            inverse = d_ref[layer]
            ph[side, step], pw[side, step] = halves(product(halves(inverse), coupling, dims))
            move = (ph[side, step], pw[side, step])
            if step == 0:
                state_ref[side] = inverse
                kh_ref[side, layer], kl_ref[side, layer] = halves(
                    (move[0].astype(F32) + move[1].astype(F32)).T
                )
                row = jnp.zeros_like(base_ref[:1, :])
            else:
                carried = product((kh_ref[side, before], kl_ref[side, before]), move, NT)
                kh_ref[side, layer], kl_ref[side, layer] = halves(carried)
                half_way = product(move, halves(state_ref[side]), NN)
                updated = inverse + product(halves(half_way), move, NT)
                state_ref[side] = updated
                row = diagonal_row(updated)
                if layer not in seen:
                    row = row - diagonal_row(inverse)
            if layer in seen:
                row = row + base_ref[layer : layer + 1, :]
            base_ref[layer : layer + 1, :] = row
            seen.add(layer)

    for side, last in ((0, layers - 1), (1, 0)):
        whole = (kh_ref[side, last].astype(F32) + kl_ref[side, last].astype(F32)).T
        map_h[side], map_l[side] = halves(whole)
    side = (place[0] >= 2).astype(jnp.int32)
    pltpu.make_async_copy(lead_hbm, lead, arrived.at[1 + layers]).wait()
    pack(send_ref, through(lead[...], side, state_ref, map_h, map_l))


def through(entering, side, state_ref, map_h, map_l):
    whole = (map_h[side], map_l[side])
    half_way = product(whole, halves(entering), NN)
    return state_ref[side] + product(halves(half_way), whole, NT)


def hop_kernel(right_at, place, received_ref, state_ref, map_h, map_l, send_ref, full):
    unpack(received_ref, full)
    side = (place[0] == right_at).astype(jnp.int32)
    pack(send_ref, through(full[...], side, state_ref, map_h, map_l))


def add_corrections(side, full, base_ref, kh_ref, kl_ref, out_ref):
    entering = halves(full[...])
    for layer in range(base_ref.shape[0]):
        high, low = kh_ref[side, layer], kl_ref[side, layer]
        moved = product(entering, (high, low), NN)
        carried = high.astype(F32) + low.astype(F32)
        row = jnp.sum(moved * carried, axis=0, keepdims=True)
        out_ref[layer : layer + 1, :] = base_ref[layer : layer + 1, :] + row


def first_kernel(
    place, received_ref, lead_hbm, lead_r_hbm, base_ref, kh_ref, kl_ref, out_ref, full
):
    segment = place[0]

    @pl.when(segment == 0)
    def _():
        pltpu.sync_copy(lead_hbm, full)

    @pl.when(segment == 3)
    def _():
        pltpu.sync_copy(lead_r_hbm, full)

    @pl.when((segment == 1) | (segment == 2))
    def _():
        unpack(received_ref, full)

    side = (segment >= 2).astype(jnp.int32)
    add_corrections(side, full, base_ref, kh_ref, kl_ref, out_ref)


def second_kernel(
    place, slot, weights, third_ref, second_ref, base_ref, kh_ref, kl_ref, out_ref, full, rows_ref
):
    segment = place[0]

    @pl.when((segment == 0) | (segment == 3))
    def _():
        unpack(third_ref, full)

    @pl.when((segment == 1) | (segment == 2))
    def _():
        unpack(second_ref, full)

    side = (segment < 2).astype(jnp.int32)
    add_corrections(side, full, base_ref, kh_ref, kl_ref, rows_ref)
    weighted = rows_ref[...] * weights[slot[0]]
    for peer in range(out_ref.shape[0]):
        out_ref[peer] = weighted


def fan_kernel(pieces_ref, out_ref):
    total = pieces_ref[0]
    for peer in range(1, pieces_ref.shape[0]):
        total = total + pieces_ref[peer]
    for peer in range(out_ref.shape[0]):
        out_ref[peer] = total


DEPTH = 3


def edges_kernel(
    doping_hbm, screening_hbm, doping_ref, screening_ref, high_ref, low_ref, arrived
):
    own = doping_hbm.shape[0]
    near = DEPTH - 1
    moves = [
        (doping_hbm, doping_ref),
        (screening_hbm, screening_ref),
        (doping_hbm.at[pl.ds(own - DEPTH, DEPTH)], high_ref.at[pl.ds(0, DEPTH)]),
        (screening_hbm.at[pl.ds(own - near, near)], high_ref.at[pl.ds(DEPTH, near)]),
        (doping_hbm.at[pl.ds(0, DEPTH)], low_ref.at[pl.ds(0, DEPTH)]),
        (screening_hbm.at[pl.ds(0, near)], low_ref.at[pl.ds(DEPTH, near)]),
    ]
    copies = [pltpu.make_async_copy(*move, arrived.at[i]) for i, move in enumerate(moves)]
    for copy in copies:
        copy.start()
    for copy in copies:
        copy.wait()


def krylov_kernel(
    place, plane_of, pieces_ref, doping_ref, screening_ref, below_ref, above_ref,
    own_rows_ref, basis_ref, sums_ref, src, one, two, density_ref,
):
    slab, last_slab = place[1], place[2]
    layers = pieces_ref.shape[1]
    segments = plane_of.shape[0] // layers
    for segment in range(segments):
        rows = pieces_ref[segment]
        for piece in range(segments + segment, pieces_ref.shape[0], segments):
            rows = rows + pieces_ref[piece]
        density_ref[segment * layers : (segment + 1) * layers, :] = rows
    own_rows_ref[...] = density_ref[pl.ds(pl.multiple_of(place[0] * layers, layers), layers), :]
    depth, own = DEPTH, basis_ref.shape[1]
    y_cells, z_cells = doping_ref.shape[1:]
    rows, cols = square_iota(y_cells)
    orbitals = density_ref.shape[1]
    inside_low = jnp.where(slab == 0, 0.0, 1.0)
    inside_high = jnp.where(slab == last_slab, 0.0, 1.0)
    for i in range(depth):
        src[i] = below_ref[i] * -inside_low
        src[depth + own + i] = above_ref[i] * -inside_high
    for i in range(own):
        src[depth + i] = -doping_ref[i]
    first_plane = slab * own - depth

    @pl.loop(0, plane_of.shape[0])
    def _(layer):
        at = plane_of[layer] - first_plane

        @pl.when((at >= 0) & (at < own + 2 * depth))
        def _():
            width = 16
            row = jnp.broadcast_to(density_ref[pl.ds(layer, 1), :], (y_cells, orbitals))
            yy = lax.broadcasted_iota(jnp.int32, (y_cells, orbitals), 0)
            mm = lax.broadcasted_iota(jnp.int32, (y_cells, orbitals), 1)
            spread = jnp.where(mm // width == yy // (y_cells // width), row, 0.0)
            zz = lax.broadcasted_iota(jnp.int32, (orbitals, z_cells), 1)
            mz = lax.broadcasted_iota(jnp.int32, (orbitals, z_cells), 0)
            pick = (mz % width == zz // (z_cells // width)).astype(F32).astype(BF16)
            high, low = halves(spread)
            lowest = (spread - high.astype(F32) - low.astype(F32)).astype(BF16)
            dot = functools.partial(
                lax.dot_general, dimension_numbers=NN, preferred_element_type=F32
            )
            src[at] = src[at] + (dot(high, pick) + (dot(low, pick) + dot(lowest, pick)))

    def screen(i):
        if i < depth:
            return below_ref[i + 2]
        if i < depth + own:
            return screening_ref[i - depth]
        return above_ref[i - own]

    def shifted_operator(ref, i):
        plane = ref[i]
        beside = ref[i - 1] + ref[i + 1]
        beside = beside + jnp.where(rows == 0, 0.0, pltpu.roll(plane, 1, 0))
        beside = beside + jnp.where(rows == y_cells - 1, 0.0, pltpu.roll(plane, y_cells - 1, 0))
        beside = beside + jnp.where(cols == 0, 0.0, pltpu.roll(plane, 1, 1))
        beside = beside + jnp.where(cols == z_cells - 1, 0.0, pltpu.roll(plane, z_cells - 1, 1))
        return (screen(i) + (6.0 - SHIFT)) * plane - beside

    def masked(i, plane):
        if i < depth:
            return plane * inside_low
        if i >= depth + own:
            return plane * inside_high
        return plane

    for i in range(1, own + 2 * depth - 1):
        one[i] = masked(i, shifted_operator(src, i))
    for i in range(2, own + 2 * depth - 2):
        two[i] = masked(i, shifted_operator(one, i))
    totals = [jnp.zeros((y_cells, z_cells), F32) for _ in range(6)]
    for i in range(depth, depth + own):
        three = shifted_operator(two, i)
        v = (src[i], one[i], two[i], three)
        for k in range(4):
            basis_ref[k, i - depth] = v[k]
        for k in range(6):
            totals[k] = totals[k] + v[k // 2] * v[k - k // 2]
    lane = lax.broadcasted_iota(jnp.int32, (1, z_cells), 1)
    out = jnp.zeros((1, z_cells), F32)
    for k in range(6):
        total = jnp.sum(jnp.sum(totals[k], axis=0, keepdims=True), axis=1, keepdims=True)
        out = out + jnp.where(lane == k, total, 0.0)
    for peer in range(sums_ref.shape[0]):
        sums_ref[peer] = out


def finish_kernel(sums_ref, basis_ref, potential_ref, residual_ref):
    total = jnp.sum(sums_ref[...], axis=0)
    lane = lax.broadcasted_iota(jnp.int32, total.shape, 1)
    m = [jnp.sum(jnp.where(lane == k, total, 0.0), axis=1, keepdims=True) for k in range(6)]

    def inner(a, b):
        terms = [x * y * m[i + j] for i, x in enumerate(a) for j, y in enumerate(b)]
        return functools.reduce(lambda p, q: p + q, terms)

    def applied(c):
        moved = [SHIFT * x for x in c] + [c[-1]]
        for i in range(len(c) - 1):
            moved[i + 1] = moved[i + 1] + c[i]
        return moved

    def plus(a, scale, b):
        n = max(len(a), len(b))
        a = list(a) + [None] * (n - len(a))
        b = list(b) + [None] * (n - len(b))
        return [
            x if y is None else (scale * y if x is None else x + scale * y) for x, y in zip(a, b)
        ]

    unit = jnp.ones_like(m[0])
    residual = [unit]
    direction = [unit]
    potential = []
    norm = m[0]
    for iteration in range(3):
        image = applied(direction)
        step = norm / inner(direction, image)
        potential = plus(potential, step, direction)
        residual = plus(residual, -step, image)
        if iteration < 2:
            following = inner(residual, residual)
            direction = plus(residual, following / norm, direction)
            norm = following
    for i in range(potential_ref.shape[0]):
        v = [basis_ref[k, i] for k in range(4)]
        potential_ref[i] = potential[0] * v[0] + potential[1] * v[1] + potential[2] * v[2]
        residual_ref[i] = (
            residual[0] * v[0] + residual[1] * v[1] + residual[2] * v[2] + residual[3] * v[3]
        )


def call(kernel, out_shape, in_specs, scratch=(), flops=0, out_specs=None, name=None):
    return pl.pallas_call(
        kernel,
        out_shape=out_shape,
        in_specs=in_specs,
        out_specs=jax.tree.map(lambda _: VMEM, out_shape) if out_specs is None else out_specs,
        scratch_shapes=list(scratch),
        name=name,
        cost_estimate=pl.CostEstimate(flops=flops, bytes_accessed=0, transcendentals=0),
        compiler_params=pltpu.CompilerParams(vmem_limit_bytes=40 * 2**20),
    )


def shape(*dims, dtype=F32):
    return jax.ShapeDtypeStruct(dims, dtype)


def exchange(copies, axis):
    return lax.all_to_all(copies, axis, 0, 0, tiled=True)


def body(
    layer_inverse, coupling, lead_left, lead_right, quad_weight, energy_slot, plane_of, doping, screening
):
    inverse, left, right = layer_inverse[0], lead_left[0], lead_right[0]
    layers, size = inverse.shape[0], inverse.shape[1]
    slab = lax.axis_index(ENERGY_LAYER)
    slabs = lax.axis_size(ENERGY_LAYER)
    place = jnp.stack([lax.axis_index(LAYER), slab, jnp.int32(slabs - 1)]).astype(jnp.int32)
    own, ny, nz = doping.shape

    far = functools.partial(pltpu.with_memory_space_constraint, memory_space=pltpu.HBM)
    send, base, state, map_h, map_l, kh, kl = call(
        chain_kernel,
        (
            shape(PACKED, HALF), shape(layers, size), shape(2, size, size),
            shape(2, size, size, dtype=BF16), shape(2, size, size, dtype=BF16),
            shape(2, layers, size, size, dtype=BF16), shape(2, layers, size, size, dtype=BF16),
        ),
        [SMEM, HBM, HBM, HBM, HBM],
        [
            pltpu.VMEM((layers, size, size), F32), pltpu.VMEM((size, size), F32),
            pltpu.VMEM((size, size), F32),
            *[pltpu.VMEM((2, layers, size, size), BF16)] * 2,
            pltpu.SemaphoreType.DMA((layers + 2,)),
        ],
        flops=5 * 10**9, name="chain",
    )(place, far(inverse), far(coupling), far(left), far(right))

    def hop(received, right_at):
        return call(
            functools.partial(hop_kernel, right_at), shape(PACKED, HALF),
            [SMEM, VMEM, VMEM, VMEM, VMEM], [pltpu.VMEM((size, size), F32)],
            flops=2 * 10**8, name=f"hop_{right_at}",
        )(place, received, state, map_h, map_l)

    swap = [(0, 1), (1, 0), (2, 3), (3, 2)]
    first = lax.ppermute(send, LAYER, swap)
    with jax.named_scope("middle"):
        second = lax.ppermute(hop(first, 2), LAYER, [(0, 0), (1, 2), (2, 1), (3, 3)])
    planes, screens, high_edge, low_edge = call(
        edges_kernel,
        (shape(own, ny, nz), shape(own, ny, nz), shape(5, ny, nz), shape(5, ny, nz)),
        [HBM, HBM], [pltpu.SemaphoreType.DMA((6,))],
        flops=10**8, name="edges",
    )(far(doping), far(screening))
    once = call(
        first_kernel, shape(layers, size), [SMEM, VMEM, HBM, HBM, VMEM, VMEM, VMEM],
        [pltpu.VMEM((size, size), F32)],
        flops=5 * 10**8, name="first",
    )(place, first, far(left), far(right), base, kh, kl)
    second, once, planes, screens, high_edge, low_edge = lax.optimization_barrier(
        (second, once, planes, screens, high_edge, low_edge)
    )
    third = lax.ppermute(hop(second, 1), LAYER, swap)
    third, high_edge, low_edge = lax.optimization_barrier((third, high_edge, low_edge))
    up = [(i, (i + 1) % slabs) for i in range(slabs)]
    down = [(j, i) for i, j in up]
    below = lax.ppermute(high_edge, ENERGY_LAYER, up)
    above = lax.ppermute(low_edge, ENERGY_LAYER, down)
    partial = call(
        second_kernel, shape(lax.axis_size(DEEP), layers, size), [SMEM] * 3 + [VMEM] * 5,
        [pltpu.VMEM((size, size), F32), pltpu.VMEM((layers, size), F32)],
        flops=5 * 10**8, name="second",
    )(place, energy_slot, quad_weight, third, second, once, kh, kl)
    along_z = exchange(partial, DEEP)
    fanned = call(
        fan_kernel, shape(lax.axis_size(ACROSS), layers, size), [VMEM], flops=10**6, name="fan"
    )(along_z)
    fanned, below, above = lax.optimization_barrier((fanned, below, above))
    pieces = exchange(fanned, ACROSS)

    own_rows, basis, sums = call(
        krylov_kernel,
        (shape(layers, size), shape(4, own, ny, nz), shape(slabs, 1, nz)),
        [SMEM, SMEM] + [VMEM] * 5,
        [pltpu.VMEM((own + 6, ny, nz), F32)] * 3 + [pltpu.VMEM((plane_of.shape[0], size), F32)],
        flops=10**6, name="krylov",
    )(place, plane_of, pieces, planes, screens, below, above)
    all_sums = exchange(sums, ENERGY_LAYER)
    potential, residual = call(
        finish_kernel, (shape(own, ny, nz), shape(own, ny, nz)), [VMEM] * 2,
        flops=10**6, name="finish",
    )(all_sums, basis)
    return own_rows, potential, residual


def solution(mesh):
    split = Mesh(
        mesh.devices.reshape(4, 2, 8, 2, 2),
        ("energy_0", "energy_1", "energy_2", "layer_0", "layer_1"),
    )
    in_specs = (
        P(ENERGY, LAYER, None, None),
        P(),
        P(ENERGY, None, None),
        P(ENERGY, None, None),
        P(),
        P(ENERGY),
        P(),
        P(ENERGY_LAYER, None, None),
        P(ENERGY_LAYER, None, None),
    )
    out_specs = (P(LAYER, None), P(ENERGY_LAYER, None, None), P(ENERGY_LAYER, None, None))
    return jax.shard_map(body, mesh=split, in_specs=in_specs, out_specs=out_specs, check_vma=False)
```
